256 devices in a mesh: seq: 256 (over z, x, y, core).
Axes of the slice: x: 4, y: 4, z: 8, core: 2. Of those that a mesh axis runs over, the one named last changes fastest.
Arguments:
- queries: bfloat16 [32768, 4096], P('seq'), may hold values from -48 to 48, as said below
- keys: bfloat16 [32768, 512], P('seq'), may hold values from -6 to 6, as said below
- values: bfloat16 [32768, 512], P('seq'), may hold values from -6 to 6
Outputs:
- attended: bfloat16 [32768, 4096], P('seq')
The draws below stay inside these ranges and needn't reach their ends.
Inputs may be any that keep to these rules, and one draw needn't show every extreme that they name: queries of every block, with 32 heads of 128 entries per token. keys of every block, with 4 heads of 128 entries per token.
All inputs are finite; a program needn't handle non-finite values.
Results may differ from the reference program's by a relative error of at most 0.0049.
Values may be sent and summed in bfloat16 or wider, within the bound.
A program may use at most 64 MiB of HBM per device.

```python
import math
import jax
import jax.numpy as jnp
from jax import lax

QUERY_HEADS = 32
KEY_VALUE_HEADS = 4
HEAD_SIZE = 128
BLOCK_TOKENS = 128
HALO = 64
CONTEXT_TOKENS = 32768
N_SEQ = 256


def shared_keys(key):
    source_tokens = jax.random.fold_in(key, 11)
    unscaled_scores = jnp.clip(jax.random.normal(source_tokens, (CONTEXT_TOKENS, KEY_VALUE_HEADS * HEAD_SIZE), jnp.float32), -6.0, 6.0)
    return unscaled_scores.astype(jnp.bfloat16)


def draw_keys(key, part):
    return shared_keys(key)


def draw_queries(key, part):
    source_tokens = jax.random.fold_in(key, 21)
    drawn = jnp.clip(jax.random.normal(source_tokens, (CONTEXT_TOKENS, QUERY_HEADS * HEAD_SIZE), jnp.float32), -6.0, 6.0)
    return drawn.astype(jnp.bfloat16)


def levels(own_key, dims, pieces, smallest, high):
    loudness = 1.0
    for dim, blocks in pieces:
        heights = jax.random.uniform(jax.random.fold_in(jax.random.fold_in(own_key, 6), dim), (blocks,), jnp.float32, smallest / len(pieces), high / len(pieces))
        loudness = loudness * jnp.repeat(jnp.exp(heights), dims[dim] // blocks).reshape((-1,) + (1,) * (len(dims) - 1 - dim))
    return loudness


def gaussian(own_key, shape, width, limit, cuts=(), held_as=jnp.bfloat16):
    factor_of = levels(own_key, shape, cuts, -0.22, 0.18) if cuts else 1.0
    drawn = jax.random.normal(own_key, shape, jnp.float32) * width * factor_of
    return jnp.minimum(jnp.maximum(drawn, -limit), limit).astype(held_as)


def setup_inputs(seed: int = 0) -> dict:
    seeds = jax.random.split(jax.random.key(seed), 4)
    queries = draw_queries(jax.random.fold_in(seeds[3], 71), 0)
    keys = draw_keys(jax.random.fold_in(seeds[3], 71), 0)
    values = gaussian(seeds[2], (CONTEXT_TOKENS, KEY_VALUE_HEADS * HEAD_SIZE), 1.0, 6.0, ((0, 256),))
    return {"queries": queries, "keys": keys, "values": values}


def reference(queries, keys, values):
    query_groups = QUERY_HEADS // KEY_VALUE_HEADS
    block_count = 2 * BLOCK_TOKENS + HALO
    scale = 1.0 / math.sqrt(HEAD_SIZE)
    anchor_keys = keys[:BLOCK_TOKENS]
    anchor_values = values[:BLOCK_TOKENS]
    row_ids = jnp.arange(BLOCK_TOKENS, dtype=jnp.int32)[:, None]
    col_ids = jnp.arange(BLOCK_TOKENS, dtype=jnp.int32)[None, :]

    def one_block(block):
        start = (block * BLOCK_TOKENS).astype(jnp.int32)
        halo_start = jnp.maximum(start - HALO, 0).astype(jnp.int32)
        query_matrix = lax.dynamic_slice_in_dim(queries, start, BLOCK_TOKENS, 0).astype(jnp.float32)
        query_matrix = query_matrix.reshape(BLOCK_TOKENS, KEY_VALUE_HEADS, query_groups, HEAD_SIZE)
        local_keys = lax.dynamic_slice_in_dim(keys, start, BLOCK_TOKENS, 0)
        local_values = lax.dynamic_slice_in_dim(values, start, BLOCK_TOKENS, 0)
        halo_keys = lax.dynamic_slice_in_dim(keys, halo_start, HALO, 0)
        halo_values = lax.dynamic_slice_in_dim(values, halo_start, HALO, 0)
        joined_keys = jnp.concatenate([anchor_keys, halo_keys, local_keys], axis=0).astype(jnp.float32).reshape(block_count, KEY_VALUE_HEADS, HEAD_SIZE)
        joined_values = jnp.concatenate([anchor_values, halo_values, local_values], axis=0).astype(jnp.float32).reshape(block_count, KEY_VALUE_HEADS, HEAD_SIZE)
        scores = jnp.einsum('thgd,khd->hgtk', query_matrix, joined_keys) * scale
        visible = jnp.concatenate([jnp.broadcast_to(block > 0, (BLOCK_TOKENS, BLOCK_TOKENS)), jnp.broadcast_to(block > 0, (BLOCK_TOKENS, HALO)), col_ids <= row_ids], axis=1)
        scores = jnp.where(visible, scores, jnp.float32(-1e+30))
        highest = lax.optimization_barrier(jnp.max(scores, axis=-1, keepdims=True))
        expo = jnp.exp(scores - highest)
        weights = (expo / lax.optimization_barrier(jnp.sum(expo, axis=-1, keepdims=True))).astype(jnp.bfloat16)
        mixed = jnp.einsum('hgtk,khd->thgd', weights.astype(jnp.float32), joined_values)
        return mixed.reshape(BLOCK_TOKENS, QUERY_HEADS * HEAD_SIZE).astype(jnp.bfloat16)
    blocks = lax.map(one_block, jnp.arange(N_SEQ, dtype=jnp.int32))
    return blocks.reshape(CONTEXT_TOKENS, QUERY_HEADS * HEAD_SIZE)
```

```python
import functools
import math

import jax
import jax.numpy as jnp
from jax import lax
from jax.experimental import pallas as pl
from jax.experimental.pallas import tpu as pltpu
from jax.sharding import PartitionSpec as P

HEADS = 32
KV = 4
D = 128
T = 128
HALO = 64
Z, X, Y = 8, 4, 4
NDEV = 256
PIECES = 2 * KV
SCALE = 1.0 / math.sqrt(D)
NEG = -1e30
UNITS = 16
SIZES = {"z": Z, "x": X, "y": Y}
ORDERS = ("zxy", "xyz", "yxz")
PIECE_ORDER = (0, 1, 2, 1, 0, 2, 1, 2)
FAR_FIRST = {8: (4, 3, 5, 2, 6, 1, 7), 4: (2, 1, 3)}
MESH = pl.DeviceIdType.MESH


def device(c, core):
    return ((c["z"] * X + c["x"]) * Y + c["y"]) * 2 + core


def where(flag, a, b):
    return jnp.where(flag, jnp.int32(a), jnp.int32(b))


def kernel(q_ref, k_ref, v_ref, o_ref, q, kl, vl, anc, m1, acc, pa, local_sem, q_sem, anchor_sem, halo_sem, halo_send, send_sem):
    me = lax.axis_index("seq")
    core = me % 2
    c = {"y": (me // 2) % Y, "x": (me // (2 * Y)) % X, "z": me // (2 * Y * X)}
    sibling = me + 1 - 2 * core
    at0 = {a: c[a] == 0 for a in "zxy"}
    root_chip = at0["z"] & at0["x"] & at0["y"]
    root = me == 0
    relay = jnp.where(root_chip, core == 0, core == 1)
    barrier = pltpu.get_barrier_semaphore()

    def greet(target):
        pl.semaphore_signal(barrier, inc=1, device_id=(target,), device_id_type=MESH)

    @pl.when(jnp.logical_not(relay))
    def _():
        greet(sibling)

    @pl.when(me > 0)
    def _():
        greet(me - 1)

    expected = where(me < NDEV - 1, 1, 0) + where(relay, 1, 0)
    for order in ORDERS:
        a, b, d = order
        parent = dict(c)
        last = jnp.logical_not(at0[d])
        mid = jnp.logical_not(at0[b])
        parent[d] = jnp.int32(0)
        parent[b] = where(last, c[b], 0)
        parent[a] = where(last | mid, c[a], 0)
        to_root = at0["z"] if False else (parent["z"] + parent["x"] + parent["y"]) == 0
        owner = device(parent, where(to_root, 0, 1))

        @pl.when(relay & jnp.logical_not(root))
        def _():
            greet(owner)

        expected = expected + where(relay & at0[d], SIZES[d] - 1, 0)
        expected = expected + where(relay & at0[d] & at0[b], SIZES[b] - 1, 0)
        expected = expected + where(root, SIZES[a] - 1, 0)

    locals_ = []
    for h in range(KV):
        cols = pl.ds(h * D, D)
        locals_.append(pltpu.make_async_copy(k_ref.at[:, cols], kl.at[h, pl.ds(HALO, T), :], local_sem.at[h]))
        locals_.append(pltpu.make_async_copy(v_ref.at[:, cols], vl.at[h, pl.ds(HALO, T), pl.ds(0, D)], local_sem.at[KV + h]))
    roots = []
    for p in range(PIECES):
        src = (k_ref if p < KV else v_ref).at[:, pl.ds((p % KV) * D, D)]
        roots.append(pltpu.make_async_copy(src, anc.at[p], anchor_sem.at[p]))

    @pl.when(root)
    def _():
        for copy in roots:
            copy.start()

    for copy in locals_:
        copy.start()
    for g in range(HEADS):
        pltpu.make_async_copy(q_ref.at[:, pl.ds(g * D, D)], q.at[g // 2, pl.ds((g % 2) * T, T), :], q_sem).start()
    for h in range(KV):
        vl[h, :, D:] = jnp.ones((HALO + T, D), jnp.bfloat16)

    @pl.when(root)
    def _():
        for h in range(KV):
            kl[h, :HALO, :] = jnp.zeros((HALO, D), jnp.bfloat16)
            vl[h, :HALO, :D] = jnp.zeros((HALO, D), jnp.bfloat16)

    pl.semaphore_wait(barrier, expected)

    halos = []
    for h in range(KV):
        rows, cols = pl.ds(T - HALO, HALO), pl.ds(h * D, D)
        for i, (src, dst) in enumerate(((k_ref, kl), (v_ref, vl))):
            halos.append(
                pltpu.make_async_remote_copy(
                    src_ref=src.at[rows, cols],
                    dst_ref=dst.at[h, pl.ds(0, HALO), pl.ds(0, D)],
                    send_sem=halo_send.at[2 * h + i],
                    recv_sem=halo_sem.at[2 * h + i],
                    device_id=(me + 1,),
                    device_id_type=MESH,
                )
            )

    def sends(p):
        a, b, d = ORDERS[PIECE_ORDER[p]]
        out = []
        slot = 0
        for axis, flag in ((a, root), (b, relay & at0[b] & at0[d]), (d, relay & at0[d])):
            for off in FAR_FIRST[SIZES[axis]]:
                to = dict(c)
                to[axis] = (c[axis] + off) % SIZES[axis]
                out.append((flag, slot, device(to, 1)))
                slot += 1
        out.append((relay, slot, sibling))
        return out

    def remote(p, slot, target):
        return pltpu.make_async_remote_copy(
            src_ref=anc.at[p],
            dst_ref=anc.at[p],
            send_sem=send_sem.at[p, slot],
            recv_sem=anchor_sem.at[p],
            device_id=(target,),
            device_id_type=MESH,
        )

    def forward(p):
        pltpu.make_async_copy(anc.at[p], anc.at[p], anchor_sem.at[p]).wait()
        for flag, slot, target in sends(p):
            @pl.when(flag)
            def _():
                remote(p, slot, target).start()

    @pl.when(root)
    def _():
        for p in range(PIECES):
            forward(p)

    @pl.when(me < NDEV - 1)
    def _():
        for copy in halos:
            copy.start()

    for copy in locals_:
        copy.wait()
    pltpu.make_async_copy(q, q, q_sem).wait()

    @pl.when(me > 0)
    def _():
        for copy in halos:
            copy.wait_recv()

    columns = lax.broadcasted_iota(jnp.int32, (2 * T, HALO + T), 1)
    rows = lax.broadcasted_iota(jnp.int32, (2 * T, HALO + T), 0) % T
    seen = (columns - HALO) <= rows
    seen = seen & ((columns >= HALO) | (me > 0))

    def near(u, _):
        h = u // (UNITS // KV)
        s = lax.dot_general(q[u], kl[h], (((1,), (1,)), ((), ())), preferred_element_type=jnp.float32) * SCALE
        s = jnp.where(seen, s, NEG)
        top = jnp.max(s, axis=-1, keepdims=True)
        p = jnp.exp(s - top).astype(jnp.bfloat16)
        m1[u] = jnp.broadcast_to(top, (2 * T, D))
        acc[u] = jnp.dot(p, vl[h], preferred_element_type=jnp.float32)
        return 0

    lax.fori_loop(0, UNITS, near, 0)

    @pl.when(jnp.logical_not(root))
    def _():
        for p in range(PIECES):
            forward(p)

    def far_keys(u, _):
        h = u // (UNITS // KV)
        s = lax.dot_general(q[u], anc[h], (((1,), (1,)), ((), ())), preferred_element_type=jnp.float32) * SCALE
        s = jnp.where(me > 0, s, NEG)
        old = m1[u]
        top = jnp.maximum(jnp.max(s, axis=-1, keepdims=True), old)
        pa[u] = jnp.exp(s - top).astype(jnp.bfloat16)
        fade = jnp.exp(old - top)
        acc[u] = acc[u] * jnp.concatenate([fade, fade], axis=1)
        return 0

    lax.fori_loop(0, UNITS, far_keys, 0)

    def far_values(u, _):
        h = u // (UNITS // KV)
        v = jnp.concatenate([anc[KV + h], jnp.ones((T, D), jnp.bfloat16)], axis=1)
        total = acc[u] + jnp.dot(pa[u], v, preferred_element_type=jnp.float32)
        out = (total[:, :D] / total[:, D:]).astype(jnp.bfloat16)
        o_ref[:, pl.ds(pl.multiple_of(u * 2 * D, D), D)] = out[:T]
        o_ref[:, pl.ds(pl.multiple_of(u * 2 * D + D, D), D)] = out[T:]
        return 0

    lax.fori_loop(0, UNITS, far_values, 0)

    @pl.when(me < NDEV - 1)
    def _():
        for copy in halos:
            copy.wait_send()

    for p in range(PIECES):
        for flag, slot, target in sends(p):
            @pl.when(flag)
            def _():
                remote(p, slot, target).wait_send()


def shards(queries, keys, values):
    return pl.pallas_call(
        kernel,
        out_shape=jax.ShapeDtypeStruct((T, HEADS * D), jnp.bfloat16),
        in_specs=[pl.BlockSpec(memory_space=pl.ANY)] * 3,
        out_specs=pl.BlockSpec(memory_space=pltpu.VMEM),
        scratch_shapes=[
            pltpu.VMEM((UNITS, 2 * T, D), jnp.bfloat16),
            pltpu.VMEM((KV, HALO + T, D), jnp.bfloat16),
            pltpu.VMEM((KV, HALO + T, 2 * D), jnp.bfloat16),
            pltpu.VMEM((PIECES, T, D), jnp.bfloat16),
            pltpu.VMEM((UNITS, 2 * T, D), jnp.float32),
            pltpu.VMEM((UNITS, 2 * T, 2 * D), jnp.float32),
            pltpu.VMEM((UNITS, 2 * T, D), jnp.bfloat16),
            pltpu.SemaphoreType.DMA((2 * KV,)),
            pltpu.SemaphoreType.DMA,
            pltpu.SemaphoreType.DMA((PIECES,)),
            pltpu.SemaphoreType.DMA((2 * KV,)),
            pltpu.SemaphoreType.DMA((2 * KV,)),
            pltpu.SemaphoreType.DMA((PIECES, 14)),
        ],
        compiler_params=pltpu.CompilerParams(collective_id=0, has_side_effects=True),
    )(queries, keys, values)


def solution(mesh):
    return jax.shard_map(
        shards,
        mesh=mesh,
        in_specs=(P("seq", None),) * 3,
        out_specs=P("seq", None),
        check_vma=False,
    )
```
